32 devices in a mesh: row: 4 (over y, x), col: 8 (over z, core).
Axes of the slice: x: 2, y: 2, z: 4, core: 2. Of those that a mesh axis runs over, the one named last changes fastest.
Arguments:
- tile_weights: bfloat16 [4, 8, 2, 128, 128], P('row', 'col'), may hold values from 0 to 4, as said below
- tile_pos: int32 [4, 8, 2, 2], P('row', 'col'), may hold values from 0 to 1, as said below
- tile_total: int32 [4, 8], P('row', 'col'), may hold values from 1 to 2, as said below
- root_ids: int32 [128], replicated, may hold values from 0 to 1023
Outputs:
- hop_level: int32 [1024, 128], P(('row', 'col'))
- path_share: float32 [1024, 128], P(('row', 'col'))
- found_per_level: float32 [4, 128], replicated
The draws below stay inside these ranges and needn't reach their ends.
Inputs may be any that keep to these rules, and one draw needn't show every extreme that they name: `tile_weights`: nonnegative; an entry is zero wherever the tile has no edge. `tile_pos`: the slots of one device name distinct tile positions; tile rows lie below 2 and tile columns below 1. `tile_total`: some device uses all 2 slots; slots at or past a device's total hold arbitrary positions and zero weights.
All inputs are finite; a program needn't handle non-finite values.
Results may differ from the reference program's by a relative error of at most 0.01.
Values may be sent and summed in bfloat16 or wider, within the bound.
A program may use at most 64 MiB of HBM per device.

```python
import jax
import jax.numpy as jnp
from jax import lax

ROOTS = 128
PV = 32
LEVELS = 4
VERTICES = 1024
ROW_BLOCK = 256
COL_BLOCK = 128
TILES_DEV = 2
N_ROW = 4
N_COL = 8


def graph_layout(key):
    base = jax.random.fold_in(key, 5)
    device_count = N_ROW * N_COL
    bit_count = (VERTICES - 1).bit_length()
    edge_count = 16 * VERTICES
    dest_ids = jnp.zeros((edge_count,), jnp.int32)
    source_ids = jnp.zeros((edge_count,), jnp.int32)
    for bit_level in range(bit_count):
        pick = jax.random.randint(jax.random.fold_in(base, bit_level), (edge_count,), 0, 100, jnp.int32)
        down_bit = (pick >= 76).astype(jnp.int32)
        right_bit = ((pick >= 57) & (pick < 76) | (pick >= 95)).astype(jnp.int32)
        dest_ids = dest_ids * 2 + down_bit
        source_ids = source_ids * 2 + right_bit
    dest_ids = dest_ids % VERTICES
    source_ids = source_ids % VERTICES
    row_tiles = ROW_BLOCK // 128
    col_tiles = COL_BLOCK // 128
    positions = row_tiles * col_tiles
    block_row = dest_ids // ROW_BLOCK
    inner_row = dest_ids % ROW_BLOCK
    block_col = source_ids // PV % N_COL
    inner_col = source_ids // (PV * N_COL) * PV + source_ids % PV
    device_ids = block_row * N_COL + block_col
    tile_ids = device_ids * positions + inner_row // 128 * col_tiles + inner_col // 128
    hits = jnp.zeros((device_count * positions,), jnp.int32).at[tile_ids].add(1)
    hits = jnp.minimum(hits, 1 << 20).reshape(device_count, positions)
    order_keys = jax.random.split(jax.random.fold_in(base, 997), device_count)
    ranks = jax.vmap(lambda one_key: jax.random.permutation(one_key, positions).astype(jnp.int32))(order_keys)
    scores = hits * positions + ranks
    _, chosen = lax.top_k(scores, TILES_DEV)
    chosen = chosen.astype(jnp.int32)
    slot_keys = jax.random.split(jax.random.fold_in(base, 1999), device_count)
    slot_order = jax.vmap(lambda one_key: jax.random.permutation(one_key, TILES_DEV).astype(jnp.int32))(slot_keys)
    chosen = jnp.take_along_axis(chosen, slot_order, axis=1)
    totals = jax.random.randint(jax.random.fold_in(base, 2999), (device_count,), 1, TILES_DEV + 1, jnp.int32)
    fullest = jax.random.randint(jax.random.fold_in(base, 3999), (), 0, device_count, jnp.int32)
    totals = totals.at[fullest].set(TILES_DEV)
    slot_index = jnp.broadcast_to(jnp.arange(TILES_DEV, dtype=jnp.int32)[None, :], (device_count, TILES_DEV))
    flat_chosen = (jnp.arange(device_count, dtype=jnp.int32)[:, None] * positions + chosen).reshape(-1)
    slot_of = jnp.full((device_count * positions,), -1, jnp.int32).at[flat_chosen].set(slot_index.reshape(-1))
    edge_slot = slot_of[tile_ids]
    keep = (edge_slot >= 0) & (edge_slot < totals[device_ids])
    cell = (device_ids * TILES_DEV + jnp.maximum(edge_slot, 0)) * 16384 + inner_row % 128 * 128 + inner_col % 128
    cell = jnp.where(keep, cell, device_count * TILES_DEV * 16384)
    return (chosen, totals, cell, edge_count)


def draw_tile_weights(key, part):
    chosen, totals, cell, edge_count = graph_layout(key)
    value_key = jax.random.fold_in(key, 77)
    values = jnp.exp(jax.random.uniform(value_key, (edge_count,), jnp.float32, jnp.log(0.5), jnp.log(2.0)))
    flat = jnp.zeros((N_ROW * N_COL * TILES_DEV * 16384,), jnp.bfloat16)
    flat = flat.at[cell].max(values.astype(jnp.bfloat16), mode='drop')
    return flat.reshape(N_ROW, N_COL, TILES_DEV, 128, 128)


def draw_tile_pos(key, part):
    chosen, totals, cell, edge_count = graph_layout(key)
    col_tiles = COL_BLOCK // 128
    stacked = jnp.stack([chosen // col_tiles, chosen % col_tiles], axis=1)
    return stacked.reshape(N_ROW, N_COL, 2, TILES_DEV).astype(jnp.int32)


def draw_tile_total(key, part):
    chosen, totals, cell, edge_count = graph_layout(key)
    return totals.reshape(N_ROW, N_COL).astype(jnp.int32)


def touch_ends(values, rng, low, high):
    longest = values.shape.index(max(values.shape))
    spots = []
    for shift in (0, 1):
        where = [jax.random.randint(jax.random.fold_in(rng, axis), (), 0, length) for axis, length in enumerate(values.shape)]
        where[longest] = (where[longest] + shift) % values.shape[longest]
        spots.append(tuple(where))
    return values.at[spots[0]].set(low).at[spots[1]].set(high)


def setup_inputs(seed: int = 0) -> dict:
    arg_keys = jax.random.split(jax.random.key(seed), 5)
    tile_weights = draw_tile_weights(jax.random.fold_in(arg_keys[4], 71), 0)
    tile_pos = draw_tile_pos(jax.random.fold_in(arg_keys[4], 71), 0)
    tile_total = draw_tile_total(jax.random.fold_in(arg_keys[4], 71), 0)
    root_ids = touch_ends(jax.random.randint(arg_keys[3], (ROOTS,), 0, VERTICES), jax.random.fold_in(arg_keys[3], 1), 0, VERTICES - 1).astype(jnp.int32)
    return {"tile_weights": tile_weights, "tile_pos": tile_pos, "tile_total": tile_total, "root_ids": root_ids}


def device_partial(frontier, tiles, dest_tiles, source_tiles, limit, col_index):
    offsets = jnp.arange(128, dtype=jnp.int32)

    def advance(total, slot):
        tile = tiles[slot].astype(jnp.float32)
        local_cols = source_tiles[slot] * 128 + offsets
        global_cols = ((local_cols // PV) * N_COL + col_index) * PV + local_cols % PV
        block = frontier[global_cols].astype(jnp.float32)
        contrib = jnp.dot(tile, block, precision=lax.Precision.HIGHEST)
        contrib = contrib * (slot < limit).astype(jnp.float32)
        start = (dest_tiles[slot] * 128).astype(jnp.int32)
        current = lax.dynamic_slice_in_dim(total, start, 128, 0)
        return lax.dynamic_update_slice_in_dim(total, current + contrib, start, 0), None

    total = jnp.zeros((PV * N_COL, ROOTS), jnp.float32)
    total, _ = lax.scan(advance, total, jnp.arange(TILES_DEV, dtype=jnp.int32))
    return total


def propagate(frontier, dev_tiles, dev_dest, dev_source, dev_total):
    row_block = PV * N_COL
    arrived = jnp.zeros((PV * N_ROW * N_COL, ROOTS), jnp.float32)

    def each_device(carry, device):
        row_index = device // N_COL
        col_index = device % N_COL
        partial_value = device_partial(frontier, dev_tiles[device], dev_dest[device], dev_source[device], dev_total[device], col_index)
        rounded = lax.optimization_barrier(partial_value.astype(jnp.bfloat16)).astype(jnp.float32)
        start = (row_index * row_block).astype(jnp.int32)
        current = lax.dynamic_slice_in_dim(carry, start, row_block, 0)
        return lax.dynamic_update_slice_in_dim(carry, current + rounded, start, 0), None

    arrived, _ = lax.scan(each_device, arrived, jnp.arange(N_ROW * N_COL, dtype=jnp.int32))
    return arrived


def reference(tile_weights, tile_pos, tile_total, root_ids):
    device_count = N_ROW * N_COL
    dev_tiles = tile_weights.reshape(device_count, TILES_DEV, 128, 128)
    dev_dest = tile_pos[:, :, 0, :].reshape(device_count, TILES_DEV).astype(jnp.int32)
    dev_source = tile_pos[:, :, 1, :].reshape(device_count, TILES_DEV).astype(jnp.int32)
    dev_total = tile_total.reshape(device_count).astype(jnp.int32)
    vertex_ids = jnp.arange(PV * N_ROW * N_COL, dtype=jnp.int32)
    is_root = vertex_ids[:, None] == root_ids[None, :]
    path_now = is_root.astype(jnp.float32)
    kept_weight = path_now
    hop_level = jnp.where(is_root, 0, LEVELS + 1).astype(jnp.int32)
    found_counts = []
    found_totals = []
    for level_num in range(LEVELS):
        frontier = path_now.astype(jnp.bfloat16)
        arrived = propagate(frontier, dev_tiles, dev_dest, dev_source, dev_total)
        newly = (arrived > 0) & (hop_level == LEVELS + 1)
        path_now = jnp.where(newly, arrived, jnp.float32(0.0))
        hop_level = jnp.where(newly, jnp.int32(level_num + 1), hop_level)
        kept_weight = kept_weight + path_now
        found_counts.append(jnp.sum(newly.astype(jnp.float32), axis=0))
        found_totals.append(jnp.sum(path_now, axis=0))
    counts = jnp.stack(found_counts)
    totals = jnp.stack(found_totals)
    factor = counts / jnp.maximum(totals, 1.0)
    factor_table = jnp.concatenate([jnp.ones((1, ROOTS), jnp.float32), factor, jnp.zeros((1, ROOTS), jnp.float32)], axis=0)
    scale = jnp.zeros_like(kept_weight)
    for level_num in range(LEVELS + 2):
        scale = scale + jnp.where(hop_level == level_num, factor_table[level_num][None, :], jnp.float32(0.0))
    return hop_level, kept_weight * scale, counts
```

```python
import functools

import jax
import jax.numpy as jnp
from jax import lax
from jax.experimental import pallas as pl
from jax.experimental.pallas import tpu as pltpu
from jax.sharding import PartitionSpec as P

ROOTS = 128
PV = 32
LEVELS = 4
TILE = 128
REPLICA_LIMIT = 16 * 2**20


def tile_products(source_rows, live_tiles, dest_slots, source_slots, row_tiles):
    source_tiles = source_rows.reshape(-1, 128, source_rows.shape[1])
    blocks = source_tiles[source_slots]
    products = jnp.einsum("src,sck->srk", live_tiles, blocks, preferred_element_type=jnp.float32)
    partial_value = jnp.zeros((row_tiles, 128, source_rows.shape[1]), jnp.float32)
    partial_value = partial_value.at[dest_slots].add(products)
    return partial_value.reshape(row_tiles * 128, source_rows.shape[1])


def local(tile_weights, tile_pos, tile_total, root_ids):
    col_devices = lax.axis_size("col")
    row_index = lax.axis_index("row")
    col_index = lax.axis_index("col")
    tile_data = tile_weights[0, 0]
    positions = tile_pos[0, 0]
    slot_limit = tile_total[0, 0]
    slot_total = tile_data.shape[0]
    in_use = (jnp.arange(slot_total, dtype=jnp.int32) < slot_limit).astype(jnp.bfloat16)
    live_tiles = tile_data * in_use[:, None, None]
    dest_slots = positions[0]
    source_slots = positions[1]
    row_block = col_devices * PV
    row_tiles = row_block // 128
    state_start = (row_index * col_devices + col_index) * PV
    state_rows = PV
    vertex_ids = state_start + jnp.arange(state_rows, dtype=jnp.int32)
    is_root = vertex_ids[:, None] == root_ids[None, :]
    kept_weight = is_root.astype(jnp.float32)
    path_now = is_root.astype(jnp.bfloat16)
    hop_level = jnp.where(is_root, 0, LEVELS + 1).astype(jnp.int32)
    found_counts = []
    found_totals = []
    for level_num in range(LEVELS):
        own_front = path_now
        source_rows = lax.all_gather(own_front, "row", axis=0, tiled=True)
        partial_value = tile_products(source_rows, live_tiles, dest_slots, source_slots, row_tiles)
        arrived = lax.psum_scatter(
            partial_value.astype(jnp.bfloat16), "col", scatter_dimension=0, tiled=True
        ).astype(jnp.float32)
        newly = (arrived > 0) & (hop_level == LEVELS + 1)
        path_weight = jnp.where(newly, arrived, jnp.float32(0.0))
        hop_level = jnp.where(newly, jnp.int32(level_num + 1), hop_level)
        kept_weight = kept_weight + path_weight
        path_now = path_weight.astype(jnp.bfloat16)
        found_count = jnp.sum(newly.astype(jnp.float32), axis=0)
        found_total = jnp.sum(path_weight, axis=0)
        found_counts.append(found_count)
        found_totals.append(found_total)
    counts = jnp.stack(found_counts)
    totals = jnp.stack(found_totals)
    counts, totals = lax.psum((counts, totals), ("row", "col"))
    factor = counts / jnp.maximum(totals, 1.0)
    factor_table = jnp.concatenate(
        [jnp.ones((1, ROOTS), jnp.float32), factor, jnp.zeros((1, ROOTS), jnp.float32)], axis=0
    )
    scale = jnp.zeros_like(kept_weight)
    for level_num in range(LEVELS + 2):
        scale = scale + jnp.where(
            hop_level == level_num, factor_table[level_num][None, :], jnp.float32(0.0)
        )
    return (hop_level, kept_weight * scale, counts)


def near_order(depth):
    table = []
    for z in range(depth):
        up = z < depth / 2
        others = [other for other in range(depth) if other != z]
        table.append(sorted(others, key=lambda o: (abs(o - z), (o < z) if up else (o > z))))
    return table


def pick(table, z, step):
    value = jnp.int32(0)
    for index, entries in enumerate(table):
        value = jnp.where(z == index, jnp.int32(entries[step]), value)
    return value


def kernel(
    n_row, n_col, tiles_ref, pos_ref, total_ref, roots_ref, hop_out, share_out, counts_out,
    adj, front, hop, path, send_z, recv_z, send_n, recv_n, send_d, recv_d, send_s, recv_s, recv_sd,
):
    r = lax.axis_index("row")
    c = lax.axis_index("col")
    z, core = c // 2, c % 2
    y, x = r // 2, r % 2
    row_x, row_y, row_d = y * 2 + (1 - x), (1 - y) * 2 + x, (1 - y) * 2 + (1 - x)
    rows = (row_x, row_y)
    depth = n_col // 2
    slots = tiles_ref.shape[0]
    row_block, col_block = adj.shape[2], adj.shape[3]
    half = row_block // 2
    roots = roots_ref.shape[1]
    table = near_order(depth)

    barrier = pltpu.get_barrier_semaphore()
    others = [(r, pick(table, z, step) * 2 + core) for step in range(depth - 1)]
    others += [(row_x, c), (row_y, c), (r, z * 2 + 1 - core)]
    for device in others:
        pl.semaphore_signal(barrier, inc=1, device_id=device, device_id_type=pl.DeviceIdType.MESH)

    for tr in range(row_block // TILE):
        for tc in range(col_block // TILE):
            value = jnp.zeros((TILE, TILE), jnp.float32)
            for s in range(slots):
                here = (pos_ref[0, s] == tr) & (pos_ref[1, s] == tc) & (s < total_ref[0, 0])
                value = value + tiles_ref[s].astype(jnp.float32) * here.astype(jnp.float32)
            adj[c, r, pl.ds(tr * TILE, TILE), pl.ds(tc * TILE, TILE)] = value.astype(jnp.bfloat16)

    for rr in range(n_row):
        part = pl.ds(rr * row_block, row_block)
        ids = rr * row_block + lax.broadcasted_iota(jnp.int32, (row_block, roots), 0)
        is_root = ids == roots_ref[...]
        hop[part] = jnp.where(is_root, 0, LEVELS + 1).astype(jnp.int32)
        path[part] = is_root.astype(jnp.float32)
        for cc in range(n_col):
            front[0, pl.ds(cc * col_block + rr * PV, PV)] = (
                is_root[cc * PV:(cc + 1) * PV].astype(jnp.float32).astype(jnp.bfloat16)
            )

    pl.semaphore_wait(barrier, len(others))

    started = []

    def send(ref, send_sem, recv_sem, device):
        copy = pltpu.make_async_remote_copy(
            src_ref=ref, dst_ref=ref, send_sem=send_sem, recv_sem=recv_sem,
            device_id=device, device_id_type=pl.DeviceIdType.MESH,
        )
        copy.start()
        started.append(copy)

    def arrive(ref, send_sem, recv_sem):
        pltpu.make_async_remote_copy(
            src_ref=ref, dst_ref=ref, send_sem=send_sem, recv_sem=recv_sem,
            device_id=(r, z * 2 + 1 - core), device_id_type=pl.DeviceIdType.MESH,
        ).wait_recv()

    def block(zz, rr):
        return adj.at[zz * 2 + core, rr]

    def piece(zz, rr, h):
        return adj.at[zz * 2 + core, rr, pl.ds(h * half, half)]

    sibling = (r, z * 2 + 1 - core)

    def spread(zz):
        for axis in range(2):
            send(block(zz, r), send_n.at[axis, zz], recv_n.at[axis, zz], (rows[axis], c))

    def share_block(zz, rr):
        send(block(zz, rr), send_s.at[rr, zz], recv_s.at[rr, zz], sibling)

    def relay(zz):
        for axis in range(2):
            arrive(block(zz, rows[axis]), send_n.at[axis, zz], recv_n.at[axis, zz])
            send(piece(zz, rows[axis], axis), send_d.at[axis, zz], recv_d.at[axis, zz], (rows[1 - axis], c))
        for axis in range(2):
            share_block(zz, rows[axis])

    def finish(zz):
        for axis in range(2):
            arrive(piece(zz, row_d, axis), send_d.at[axis, zz], recv_d.at[axis, zz])
            send(piece(zz, row_d, axis), send_s.at[n_row + axis, zz], recv_sd.at[axis, zz], sibling)

    order = [z] + [pick(table, z, step) for step in range(depth - 1)]
    spread(z)
    for step in range(depth - 1):
        zz = order[step + 1]
        send(block(z, r), send_z.at[zz], recv_z.at[z], (r, zz * 2 + core))
    share_block(z, r)
    for step in range(depth):
        if step + 1 < depth:
            zz = order[step + 1]
            arrive(block(zz, r), send_z.at[zz], recv_z.at[zz])
            spread(zz)
            share_block(zz, r)
        relay(order[step])
        if step > 0:
            finish(order[step - 1])
    finish(order[depth - 1])
    for step in range(depth):
        zz = order[step]
        for rr in (r, row_x, row_y):
            arrive(adj.at[zz * 2 + 1 - core, rr], send_s.at[rr, zz], recv_s.at[rr, zz])
        for axis in range(2):
            arrive(
                adj.at[zz * 2 + 1 - core, row_d, pl.ds(axis * half, half)],
                send_s.at[n_row + axis, zz], recv_sd.at[axis, zz],
            )

    own = pl.ds(pl.multiple_of((r * n_col + c) * PV, PV), PV)
    kept = path[own]
    factors = []
    for level in range(LEVELS):
        now, later = level % 2, (level + 1) % 2
        count = jnp.zeros((1, roots), jnp.float32)
        total = jnp.zeros((1, roots), jnp.float32)
        source = front[now]
        for rr in range(n_row):
            part = pl.ds(rr * row_block, row_block)
            wide = jnp.concatenate([adj[cc, rr] for cc in range(n_col)], axis=1)
            arrived = jnp.dot(wide, source, preferred_element_type=jnp.float32)
            old = hop[part]
            newly = (arrived > 0) & (old == LEVELS + 1)
            weight = jnp.where(newly, arrived, 0.0)
            hop[part] = jnp.where(newly, level + 1, old)
            path[part] = weight
            count = count + jnp.sum(newly.astype(jnp.float32), axis=0, keepdims=True)
            total = total + jnp.sum(weight, axis=0, keepdims=True)
            narrow = weight.astype(jnp.bfloat16)
            if level + 1 < LEVELS:
                for cc in range(n_col):
                    front[later, pl.ds(cc * col_block + rr * PV, PV)] = narrow[cc * PV:(cc + 1) * PV]
        kept = kept + path[own]
        counts_out[pl.ds(level, 1)] = count
        factors.append(count / jnp.maximum(total, 1.0))
    level_own = hop[own]
    scale = jnp.where(level_own == 0, 1.0, 0.0)
    for level in range(LEVELS):
        scale = jnp.where(level_own == level + 1, factors[level], scale)
    hop_out[...] = level_own
    share_out[...] = kept * scale

    for copy in started:
        copy.wait_send()


def replicated(n_row, n_col, tile_weights, tile_pos, tile_total, root_ids):
    roots = root_ids.shape[0]
    row_block, col_block = n_col * PV, n_row * PV
    vertices = n_row * row_block
    depth = n_col // 2
    vmem = pl.BlockSpec(memory_space=pltpu.VMEM)
    smem = pl.BlockSpec(memory_space=pltpu.SMEM)
    dma = pltpu.SemaphoreType.DMA
    return pl.pallas_call(
        functools.partial(kernel, n_row, n_col),
        out_shape=(
            jax.ShapeDtypeStruct((PV, roots), jnp.int32),
            jax.ShapeDtypeStruct((PV, roots), jnp.float32),
            jax.ShapeDtypeStruct((LEVELS, roots), jnp.float32),
        ),
        in_specs=[vmem, smem, smem, vmem],
        out_specs=(vmem, vmem, vmem),
        scratch_shapes=[
            pltpu.VMEM((n_col, n_row, row_block, col_block), jnp.bfloat16),
            pltpu.VMEM((2, vertices, roots), jnp.bfloat16),
            pltpu.VMEM((vertices, roots), jnp.int32),
            pltpu.VMEM((vertices, roots), jnp.float32),
            dma((depth,)), dma((depth,)),
            dma((2, depth)), dma((2, depth)),
            dma((2, depth)), dma((2, depth)),
            dma((n_row + 2, depth)), dma((n_row, depth)), dma((2, depth)),
        ],
        compiler_params=pltpu.CompilerParams(collective_id=0, has_side_effects=True),
    )(tile_weights[0, 0], tile_pos[0, 0], tile_total, root_ids.reshape(1, roots))


def solution(mesh):
    n_row, n_col = mesh.shape["row"], mesh.shape["col"]
    vertices = n_row * n_col * PV
    placed = (P("row", "col", None, None, None), P("row", "col", None, None), P("row", "col"), P())
    body = local
    if n_row == 4 and n_col % 2 == 0 and 2 * vertices * vertices <= REPLICA_LIMIT:
        body = functools.partial(replicated, n_row, n_col)
    return jax.shard_map(
        body,
        mesh=mesh,
        in_specs=placed,
        out_specs=(P(("row", "col"), None), P(("row", "col"), None), P()),
        check_vma=False,
    )
```

```python
import functools

import jax
import jax.numpy as jnp
from jax import lax
from jax.experimental import pallas as pl
from jax.experimental.pallas import tpu as pltpu
from jax.sharding import PartitionSpec as P

ROOTS = 128
PV = 32
LEVELS = 4
TILE = 128
REPLICA_LIMIT = 16 * 2**20
LATE = 4
SENDS = 256


def tile_products(source_rows, live_tiles, dest_slots, source_slots, row_tiles):
    source_tiles = source_rows.reshape(-1, 128, source_rows.shape[1])
    blocks = source_tiles[source_slots]
    products = jnp.einsum("src,sck->srk", live_tiles, blocks, preferred_element_type=jnp.float32)
    partial_value = jnp.zeros((row_tiles, 128, source_rows.shape[1]), jnp.float32)
    partial_value = partial_value.at[dest_slots].add(products)
    return partial_value.reshape(row_tiles * 128, source_rows.shape[1])


def local(tile_weights, tile_pos, tile_total, root_ids):
    col_devices = lax.axis_size("col")
    row_index = lax.axis_index("row")
    col_index = lax.axis_index("col")
    tile_data = tile_weights[0, 0]
    positions = tile_pos[0, 0]
    slot_limit = tile_total[0, 0]
    slot_total = tile_data.shape[0]
    in_use = (jnp.arange(slot_total, dtype=jnp.int32) < slot_limit).astype(jnp.bfloat16)
    live_tiles = tile_data * in_use[:, None, None]
    dest_slots = positions[0]
    source_slots = positions[1]
    row_block = col_devices * PV
    row_tiles = row_block // 128
    state_start = (row_index * col_devices + col_index) * PV
    state_rows = PV
    vertex_ids = state_start + jnp.arange(state_rows, dtype=jnp.int32)
    is_root = vertex_ids[:, None] == root_ids[None, :]
    kept_weight = is_root.astype(jnp.float32)
    path_now = is_root.astype(jnp.bfloat16)
    hop_level = jnp.where(is_root, 0, LEVELS + 1).astype(jnp.int32)
    found_counts = []
    found_totals = []
    for level_num in range(LEVELS):
        own_front = path_now
        source_rows = lax.all_gather(own_front, "row", axis=0, tiled=True)
        partial_value = tile_products(source_rows, live_tiles, dest_slots, source_slots, row_tiles)
        arrived = lax.psum_scatter(
            partial_value.astype(jnp.bfloat16), "col", scatter_dimension=0, tiled=True
        ).astype(jnp.float32)
        newly = (arrived > 0) & (hop_level == LEVELS + 1)
        path_weight = jnp.where(newly, arrived, jnp.float32(0.0))
        hop_level = jnp.where(newly, jnp.int32(level_num + 1), hop_level)
        kept_weight = kept_weight + path_weight
        path_now = path_weight.astype(jnp.bfloat16)
        found_count = jnp.sum(newly.astype(jnp.float32), axis=0)
        found_total = jnp.sum(path_weight, axis=0)
        found_counts.append(found_count)
        found_totals.append(found_total)
    counts = jnp.stack(found_counts)
    totals = jnp.stack(found_totals)
    counts, totals = lax.psum((counts, totals), ("row", "col"))
    factor = counts / jnp.maximum(totals, 1.0)
    factor_table = jnp.concatenate(
        [jnp.ones((1, ROOTS), jnp.float32), factor, jnp.zeros((1, ROOTS), jnp.float32)], axis=0
    )
    scale = jnp.zeros_like(kept_weight)
    for level_num in range(LEVELS + 2):
        scale = scale + jnp.where(
            hop_level == level_num, factor_table[level_num][None, :], jnp.float32(0.0)
        )
    return (hop_level, kept_weight * scale, counts)


def arrival_order(depth):
    def key(z, other):
        inner = 0 < other < depth - 1
        gap = abs(other - z)
        return (gap > 1 or not inner, inner, -gap)
    return [sorted((o for o in range(depth) if o != z), key=lambda o: key(z, o)) for z in range(depth)]


def far_order(depth):
    return [sorted((o for o in range(depth) if o != z), key=lambda o: -abs(o - z)) for z in range(depth)]


def pick(table, z, step):
    value = jnp.int32(0)
    for index, entries in enumerate(table):
        value = jnp.where(z == index, jnp.int32(entries[step]), value)
    return value


def kernel(
    n_row, n_col, tiles_ref, pos_ref, total_ref, roots_ref, hop_out, share_out, counts_out,
    adj, front, hop, path, send_sem, recv_sem,
):
    r = lax.axis_index("row")
    c = lax.axis_index("col")
    z, core = c // 2, c % 2
    y, x = r // 2, r % 2
    row_x, row_y, row_d = y * 2 + (1 - x), (1 - y) * 2 + x, (1 - y) * 2 + (1 - x)
    rows = (row_x, row_y)
    depth = n_col // 2
    slots = tiles_ref.shape[0]
    row_block, col_block = adj.shape[2], adj.shape[3]
    tail = row_block // LATE // 2
    body = row_block // 2 - tail
    pieces = [(0, body), (body, body), (2 * body, tail), (2 * body + tail, tail)]
    roots = roots_ref.shape[1]
    order_table, far_table = arrival_order(depth), far_order(depth)
    order = [z] + [pick(order_table, z, step) for step in range(depth - 1)]
    far = [pick(far_table, z, step) for step in range(depth - 1)]

    barrier = pltpu.get_barrier_semaphore()
    others = [(r, far[step] * 2 + core) for step in range(depth - 1)]
    others += [(row_x, c), (row_y, c), (r, z * 2 + 1 - core)]
    for device in others:
        pl.semaphore_signal(barrier, inc=1, device_id=device, device_id_type=pl.DeviceIdType.MESH)

    for tr in range(row_block // TILE):
        for tc in range(col_block // TILE):
            value = jnp.zeros((TILE, TILE), jnp.float32)
            for s in range(slots):
                here = (pos_ref[0, s] == tr) & (pos_ref[1, s] == tc) & (s < total_ref[0, 0])
                value = value + tiles_ref[s].astype(jnp.float32) * here.astype(jnp.float32)
            adj[c, r, pl.ds(tr * TILE, TILE), pl.ds(tc * TILE, TILE)] = value.astype(jnp.bfloat16)

    for rr in range(n_row):
        part = pl.ds(rr * row_block, row_block)
        ids = rr * row_block + lax.broadcasted_iota(jnp.int32, (row_block, roots), 0)
        is_root = ids == roots_ref[...]
        hop[part] = jnp.where(is_root, 0, LEVELS + 1).astype(jnp.int32)
        path[part] = is_root.astype(jnp.float32)
        for cc in range(n_col):
            front[0, pl.ds(cc * col_block + rr * PV, PV)] = (
                is_root[cc * PV:(cc + 1) * PV].astype(jnp.float32).astype(jnp.bfloat16)
            )

    pl.semaphore_wait(barrier, len(others))

    started = []

    def each(piece, rr, zz):
        return adj.at[zz * 2 + core, rr, pl.ds(*pieces[piece])]

    def send(piece, rr, zz, device, when=None):
        copy = pltpu.make_async_remote_copy(
            src_ref=each(piece, rr, zz), dst_ref=each(piece, rr, zz),
            send_sem=send_sem.at[len(started)], recv_sem=recv_sem.at[piece, rr, zz * 2 + core],
            device_id=device, device_id_type=pl.DeviceIdType.MESH,
        )
        started.append((copy, when))
        if when is None:
            copy.start()
        else:
            pl.when(when)(copy.start)

    def arrive(piece, rr, cc):
        ref = adj.at[cc, rr, pl.ds(*pieces[piece])]
        pltpu.make_async_remote_copy(
            src_ref=ref, dst_ref=ref, send_sem=send_sem.at[0], recv_sem=recv_sem.at[piece, rr, cc],
            device_id=sibling, device_id_type=pl.DeviceIdType.MESH,
        ).wait_recv()

    def here(piece, rr, zz):
        arrive(piece, rr, zz * 2 + core)

    sibling = (r, z * 2 + 1 - core)
    is_end = (z == 0) | (z == depth - 1)

    def column(piece, rr):
        for step in range(depth - 1):
            zz = far[step]
            near = (zz == z + 1) | (zz == z - 1)
            send(piece, rr, z, (r, zz * 2 + core), is_end | near)

    def onward(piece, rr, zz):
        nxt = jnp.where(zz < z, z + 1, z - 1)
        inner = (zz > 0) & (zz < depth - 1) & (nxt >= 0) & (nxt < depth)
        nxt = jnp.where(inner, nxt, jnp.where(z > 0, 0, 1))
        send(piece, rr, zz, (r, nxt * 2 + core), inner)

    def spread(zz):
        for turn in range(2):
            for axis in range(2):
                piece = axis if turn == 0 else 1 - axis
                send(piece, r, zz, (rows[axis], c))

    def relay(base, zz):
        for axis in range(2):
            here(base + axis, rows[axis], zz)
            send(base + axis, rows[axis], zz, (rows[1 - axis], c))
        for axis in range(2):
            send(base + axis, rows[axis], zz, sibling)
        for axis in range(2):
            here(base + 1 - axis, rows[axis], zz)
            send(base + 1 - axis, rows[axis], zz, sibling)

    def finish(base, zz):
        for axis in range(2):
            here(base + axis, row_d, zz)
            send(base + axis, row_d, zz, sibling)

    def late(zz):
        for rr in (r, row_x, row_y, row_d):
            for piece in (2, 3):
                here(piece, rr, zz)
                onward(piece, rr, zz)
                send(piece, rr, zz, sibling)

    def climb(zz):
        for piece in (0, 1):
            here(piece, r, zz)
            onward(piece, r, zz)
        spread(zz)
        for piece in (0, 1):
            send(piece, r, zz, sibling)

    for turn in range(2):
        for axis in range(2):
            send(2 + (axis if turn == 0 else 1 - axis), r, z, (rows[axis], c))
    spread(z)
    for piece in range(2):
        column(piece, r)
    for piece in range(4):
        send(piece, r, z, sibling)
    relay(2, z)
    for piece in (2, 3):
        for rr in (r, row_x, row_y):
            column(piece, rr)
    relay(0, z)
    climb(order[1])
    finish(2, z)
    for piece in (2, 3):
        column(piece, row_d)
    finish(0, z)
    for step in range(1, depth):
        if step + 1 < depth:
            climb(order[step + 1])
        relay(0, order[step])
        if step > 1:
            finish(0, order[step - 1])
            late(order[step - 1])
    finish(0, order[depth - 1])
    late(order[depth - 1])
    for rr in (r, row_x, row_y, row_d):
        for step in range(depth):
            for piece in range(4):
                arrive(piece, rr, order[step] * 2 + 1 - core)

    own = pl.ds(pl.multiple_of((r * n_col + c) * PV, PV), PV)
    kept = path[own]
    factors = []
    for level in range(LEVELS):
        now, later = level % 2, (level + 1) % 2
        count = jnp.zeros((1, roots), jnp.float32)
        total = jnp.zeros((1, roots), jnp.float32)
        source = front[now]
        for rr in range(n_row):
            part = pl.ds(rr * row_block, row_block)
            wide = jnp.concatenate([adj[cc, rr] for cc in range(n_col)], axis=1)
            arrived = jnp.dot(wide, source, preferred_element_type=jnp.float32)
            old = hop[part]
            newly = (arrived > 0) & (old == LEVELS + 1)
            weight = jnp.where(newly, arrived, 0.0)
            hop[part] = jnp.where(newly, level + 1, old)
            path[part] = weight
            count = count + jnp.sum(newly.astype(jnp.float32), axis=0, keepdims=True)
            total = total + jnp.sum(weight, axis=0, keepdims=True)
            narrow = weight.astype(jnp.bfloat16)
            if level + 1 < LEVELS:
                for cc in range(n_col):
                    front[later, pl.ds(cc * col_block + rr * PV, PV)] = narrow[cc * PV:(cc + 1) * PV]
        kept = kept + path[own]
        counts_out[pl.ds(level, 1)] = count
        factors.append(count / jnp.maximum(total, 1.0))
    level_own = hop[own]
    scale = jnp.where(level_own == 0, 1.0, 0.0)
    for level in range(LEVELS):
        scale = jnp.where(level_own == level + 1, factors[level], scale)
    hop_out[...] = level_own
    share_out[...] = kept * scale

    for copy, when in started:
        if when is None:
            copy.wait_send()
        else:
            pl.when(when)(copy.wait_send)


def replicated(n_row, n_col, tile_weights, tile_pos, tile_total, root_ids):
    roots = root_ids.shape[0]
    row_block, col_block = n_col * PV, n_row * PV
    vertices = n_row * row_block
    depth = n_col // 2
    vmem = pl.BlockSpec(memory_space=pltpu.VMEM)
    smem = pl.BlockSpec(memory_space=pltpu.SMEM)
    dma = pltpu.SemaphoreType.DMA
    return pl.pallas_call(
        functools.partial(kernel, n_row, n_col),
        out_shape=(
            jax.ShapeDtypeStruct((PV, roots), jnp.int32),
            jax.ShapeDtypeStruct((PV, roots), jnp.float32),
            jax.ShapeDtypeStruct((LEVELS, roots), jnp.float32),
        ),
        in_specs=[vmem, smem, smem, vmem],
        out_specs=(vmem, vmem, vmem),
        scratch_shapes=[
            pltpu.VMEM((n_col, n_row, row_block, col_block), jnp.bfloat16),
            pltpu.VMEM((2, vertices, roots), jnp.bfloat16),
            pltpu.VMEM((vertices, roots), jnp.int32),
            pltpu.VMEM((vertices, roots), jnp.float32),
            dma((SENDS,)),
            dma((4, n_row, n_col)),
        ],
        compiler_params=pltpu.CompilerParams(collective_id=0, has_side_effects=True),
    )(tile_weights[0, 0], tile_pos[0, 0], tile_total, root_ids.reshape(1, roots))


def solution(mesh):
    n_row, n_col = mesh.shape["row"], mesh.shape["col"]
    vertices = n_row * n_col * PV
    placed = (P("row", "col", None, None, None), P("row", "col", None, None), P("row", "col"), P())
    body = local
    if n_row == 4 and n_col % 8 == 0 and 2 * vertices * vertices <= REPLICA_LIMIT:
        body = functools.partial(replicated, n_row, n_col)
    return jax.shard_map(
        body,
        mesh=mesh,
        in_specs=placed,
        out_specs=(P(("row", "col"), None), P(("row", "col"), None), P()),
        check_vma=False,
    )
```

```python
import functools

import jax
import jax.numpy as jnp
from jax import lax
from jax.experimental import pallas as pl
from jax.experimental.pallas import tpu as pltpu
from jax.sharding import PartitionSpec as P

ROOTS = 128
PV = 32
LEVELS = 4
TILE = 128
REPLICA_LIMIT = 16 * 2**20
VMEM_LIMIT = 40 * 2**20


def tile_products(source_rows, live_tiles, dest_slots, source_slots, row_tiles):
    source_tiles = source_rows.reshape(-1, 128, source_rows.shape[1])
    blocks = source_tiles[source_slots]
    products = jnp.einsum("src,sck->srk", live_tiles, blocks, preferred_element_type=jnp.float32)
    partial_value = jnp.zeros((row_tiles, 128, source_rows.shape[1]), jnp.float32)
    partial_value = partial_value.at[dest_slots].add(products)
    return partial_value.reshape(row_tiles * 128, source_rows.shape[1])


def local(tile_weights, tile_pos, tile_total, root_ids):
    col_devices = lax.axis_size("col")
    row_index = lax.axis_index("row")
    col_index = lax.axis_index("col")
    tile_data = tile_weights[0, 0]
    positions = tile_pos[0, 0]
    slot_limit = tile_total[0, 0]
    slot_total = tile_data.shape[0]
    in_use = (jnp.arange(slot_total, dtype=jnp.int32) < slot_limit).astype(jnp.bfloat16)
    live_tiles = tile_data * in_use[:, None, None]
    dest_slots = positions[0]
    source_slots = positions[1]
    row_block = col_devices * PV
    row_tiles = row_block // 128
    state_start = (row_index * col_devices + col_index) * PV
    state_rows = PV
    vertex_ids = state_start + jnp.arange(state_rows, dtype=jnp.int32)
    is_root = vertex_ids[:, None] == root_ids[None, :]
    kept_weight = is_root.astype(jnp.float32)
    path_now = is_root.astype(jnp.bfloat16)
    hop_level = jnp.where(is_root, 0, LEVELS + 1).astype(jnp.int32)
    found_counts = []
    found_totals = []
    for level_num in range(LEVELS):
        own_front = path_now
        source_rows = lax.all_gather(own_front, "row", axis=0, tiled=True)
        partial_value = tile_products(source_rows, live_tiles, dest_slots, source_slots, row_tiles)
        arrived = lax.psum_scatter(
            partial_value.astype(jnp.bfloat16), "col", scatter_dimension=0, tiled=True
        ).astype(jnp.float32)
        newly = (arrived > 0) & (hop_level == LEVELS + 1)
        path_weight = jnp.where(newly, arrived, jnp.float32(0.0))
        hop_level = jnp.where(newly, jnp.int32(level_num + 1), hop_level)
        kept_weight = kept_weight + path_weight
        path_now = path_weight.astype(jnp.bfloat16)
        found_count = jnp.sum(newly.astype(jnp.float32), axis=0)
        found_total = jnp.sum(path_weight, axis=0)
        found_counts.append(found_count)
        found_totals.append(found_total)
    counts = jnp.stack(found_counts)
    totals = jnp.stack(found_totals)
    counts, totals = lax.psum((counts, totals), ("row", "col"))
    factor = counts / jnp.maximum(totals, 1.0)
    factor_table = jnp.concatenate(
        [jnp.ones((1, ROOTS), jnp.float32), factor, jnp.zeros((1, ROOTS), jnp.float32)], axis=0
    )
    scale = jnp.zeros_like(kept_weight)
    for level_num in range(LEVELS + 2):
        scale = scale + jnp.where(
            hop_level == level_num, factor_table[level_num][None, :], jnp.float32(0.0)
        )
    return (hop_level, kept_weight * scale, counts)


def unpack(packed, hop_out, share_out, counts_out):
    hop_out[...] = packed[pl.ds(0, PV)].astype(jnp.int32)
    share_out[...] = packed[pl.ds(PV, PV)]
    counts_out[...] = packed[pl.ds(2 * PV, LEVELS)]


def kernel(
    n_row, n_col, tiles_ref, pos_ref, total_ref, roots_ref, packed,
    adj, front, hop, path, send_z, recv_z, send_n, recv_n, send_d, recv_d, send_s, recv_s, recv_sd,
):
    r = lax.axis_index("row")
    c = lax.axis_index("col")
    z, core = c // 2, c % 2
    y, x = r // 2, r % 2
    row_x, row_y, row_d = y * 2 + (1 - x), (1 - y) * 2 + x, (1 - y) * 2 + (1 - x)
    rows = (row_x, row_y)
    depth = n_col // 2
    slots = tiles_ref.shape[0]
    row_block, col_block = adj.shape[2], adj.shape[3]
    half = row_block // 2
    roots = roots_ref.shape[1]
    steps = sorted(range(1, depth), key=lambda step: min(step, depth - step))
    order = [z] + [(z + step) % depth for step in steps]

    barrier = pltpu.get_barrier_semaphore()
    others = [(r, zz * 2 + core) for zz in order[1:]]
    others += [(row_x, c), (row_y, c), (r, z * 2 + 1 - core)]
    for device in others:
        pl.semaphore_signal(barrier, inc=1, device_id=device, device_id_type=pl.DeviceIdType.MESH)

    for tr in range(row_block // TILE):
        for tc in range(col_block // TILE):
            value = jnp.zeros((TILE, TILE), jnp.float32)
            for s in range(slots):
                here = (pos_ref[0, s] == tr) & (pos_ref[1, s] == tc) & (s < total_ref[0, 0])
                value = value + tiles_ref[s].astype(jnp.float32) * here.astype(jnp.float32)
            adj[c, r, pl.ds(tr * TILE, TILE), pl.ds(tc * TILE, TILE)] = value.astype(jnp.bfloat16)

    for rr in range(n_row):
        part = pl.ds(rr * row_block, row_block)
        ids = rr * row_block + lax.broadcasted_iota(jnp.int32, (row_block, roots), 0)
        is_root = ids == roots_ref[...]
        hop[part] = jnp.where(is_root, 0, LEVELS + 1).astype(jnp.int32)
        path[part] = is_root.astype(jnp.float32)
        for cc in range(n_col):
            front[0, pl.ds(cc * col_block + rr * PV, PV)] = (
                is_root[cc * PV:(cc + 1) * PV].astype(jnp.float32).astype(jnp.bfloat16)
            )

    pl.semaphore_wait(barrier, len(others))

    started = []

    def send(ref, send_sem, recv_sem, device):
        copy = pltpu.make_async_remote_copy(
            src_ref=ref, dst_ref=ref, send_sem=send_sem, recv_sem=recv_sem,
            device_id=device, device_id_type=pl.DeviceIdType.MESH,
        )
        copy.start()
        started.append(copy)

    def arrive(ref, send_sem, recv_sem):
        pltpu.make_async_remote_copy(
            src_ref=ref, dst_ref=ref, send_sem=send_sem, recv_sem=recv_sem,
            device_id=(r, z * 2 + 1 - core), device_id_type=pl.DeviceIdType.MESH,
        ).wait_recv()

    def block(zz, rr):
        return adj.at[zz * 2 + core, rr]

    def piece(zz, rr, h):
        return adj.at[zz * 2 + core, rr, pl.ds(h * half, half)]

    sibling = (r, z * 2 + 1 - core)

    def spread(zz):
        for axis in range(2):
            send(block(zz, r), send_n.at[axis, zz], recv_n.at[axis, zz], (rows[axis], c))

    def share_block(zz, rr):
        send(block(zz, rr), send_s.at[rr, zz], recv_s.at[rr, zz], sibling)

    def relay(zz):
        for axis in range(2):
            arrive(block(zz, rows[axis]), send_n.at[axis, zz], recv_n.at[axis, zz])
            send(piece(zz, rows[axis], axis), send_d.at[axis, zz], recv_d.at[axis, zz], (rows[1 - axis], c))
        for axis in range(2):
            share_block(zz, rows[axis])

    def finish(zz):
        for axis in range(2):
            arrive(piece(zz, row_d, axis), send_d.at[axis, zz], recv_d.at[axis, zz])
            send(piece(zz, row_d, axis), send_s.at[n_row + axis, zz], recv_sd.at[axis, zz], sibling)

    spread(z)
    for step in range(depth - 1):
        zz = order[step + 1]
        send(block(z, r), send_z.at[zz], recv_z.at[z], (r, zz * 2 + core))
    share_block(z, r)
    for step in range(depth):
        if step + 1 < depth:
            zz = order[step + 1]
            arrive(block(zz, r), send_z.at[zz], recv_z.at[zz])
            spread(zz)
            share_block(zz, r)
        relay(order[step])
        if step > 0:
            finish(order[step - 1])
    finish(order[depth - 1])
    for step in range(depth):
        zz = order[step]
        for rr in (r, row_x, row_y):
            arrive(adj.at[zz * 2 + 1 - core, rr], send_s.at[rr, zz], recv_s.at[rr, zz])
        for axis in range(2):
            arrive(
                adj.at[zz * 2 + 1 - core, row_d, pl.ds(axis * half, half)],
                send_s.at[n_row + axis, zz], recv_sd.at[axis, zz],
            )

    own = pl.ds(pl.multiple_of((r * n_col + c) * PV, PV), PV)
    kept = path[own]
    factors = []
    for level in range(LEVELS):
        now, later = level % 2, (level + 1) % 2
        count = jnp.zeros((1, roots), jnp.float32)
        total = jnp.zeros((1, roots), jnp.float32)
        source = front[now]
        for rr in range(n_row):
            part = pl.ds(rr * row_block, row_block)
            wide = jnp.concatenate([adj[cc, rr] for cc in range(n_col)], axis=1)
            arrived = jnp.dot(wide, source, preferred_element_type=jnp.float32)
            old = hop[part]
            newly = (arrived > 0) & (old == LEVELS + 1)
            weight = jnp.where(newly, arrived, 0.0)
            hop[part] = jnp.where(newly, level + 1, old)
            path[part] = weight
            count = count + jnp.sum(newly.astype(jnp.float32), axis=0, keepdims=True)
            total = total + jnp.sum(weight, axis=0, keepdims=True)
            narrow = weight.astype(jnp.bfloat16)
            if level + 1 < LEVELS:
                for cc in range(n_col):
                    front[later, pl.ds(cc * col_block + rr * PV, PV)] = narrow[cc * PV:(cc + 1) * PV]
        kept = kept + path[own]
        packed[pl.ds(2 * PV + level, 1)] = count
        factors.append(count / jnp.maximum(total, 1.0))
    level_own = hop[own]
    scale = jnp.where(level_own == 0, 1.0, 0.0)
    for level in range(LEVELS):
        scale = jnp.where(level_own == level + 1, factors[level], scale)
    packed[pl.ds(0, PV)] = level_own.astype(jnp.float32)
    packed[pl.ds(PV, PV)] = kept * scale

    for copy in started:
        copy.wait_send()


def replicated(n_row, n_col, tile_weights, tile_pos, tile_total, root_ids):
    roots = root_ids.shape[0]
    row_block, col_block = n_col * PV, n_row * PV
    vertices = n_row * row_block
    depth = n_col // 2
    vmem = pl.BlockSpec(memory_space=pltpu.VMEM)
    smem = pl.BlockSpec(memory_space=pltpu.SMEM)
    dma = pltpu.SemaphoreType.DMA
    packed = pl.pallas_call(
        functools.partial(kernel, n_row, n_col),
        out_shape=jax.ShapeDtypeStruct((2 * PV + LEVELS, roots), jnp.float32),
        in_specs=[vmem, smem, smem, vmem],
        out_specs=vmem,
        scratch_shapes=[
            pltpu.VMEM((n_col, n_row, row_block, col_block), jnp.bfloat16),
            pltpu.VMEM((2, vertices, roots), jnp.bfloat16),
            pltpu.VMEM((vertices, roots), jnp.int32),
            pltpu.VMEM((vertices, roots), jnp.float32),
            dma((depth,)), dma((depth,)),
            dma((2, depth)), dma((2, depth)),
            dma((2, depth)), dma((2, depth)),
            dma((n_row + 2, depth)), dma((n_row, depth)), dma((2, depth)),
        ],
        compiler_params=pltpu.CompilerParams(collective_id=0, has_side_effects=True, vmem_limit_bytes=VMEM_LIMIT),
    )(tile_weights[0, 0], tile_pos[0, 0], tile_total, root_ids.reshape(1, roots))
    return pl.pallas_call(
        unpack,
        out_shape=(
            jax.ShapeDtypeStruct((PV, roots), jnp.int32),
            jax.ShapeDtypeStruct((PV, roots), jnp.float32),
            jax.ShapeDtypeStruct((LEVELS, roots), jnp.float32),
        ),
        in_specs=[vmem],
        out_specs=(vmem, vmem, vmem),
        compiler_params=pltpu.CompilerParams(vmem_limit_bytes=2**20),
    )(packed)


def solution(mesh):
    n_row, n_col = mesh.shape["row"], mesh.shape["col"]
    vertices = n_row * n_col * PV
    placed = (P("row", "col", None, None, None), P("row", "col", None, None), P("row", "col"), P())
    body = local
    if n_row == 4 and n_col % 2 == 0 and 2 * vertices * vertices <= REPLICA_LIMIT:
        body = functools.partial(replicated, n_row, n_col)
    return jax.shard_map(
        body,
        mesh=mesh,
        in_specs=placed,
        out_specs=(P(("row", "col"), None), P(("row", "col"), None), P()),
        check_vma=False,
    )
```

```python
import functools

import jax
import jax.numpy as jnp
from jax import lax
from jax.experimental import pallas as pl
from jax.experimental.pallas import tpu as pltpu
from jax.sharding import PartitionSpec as P

ROOTS = 128
PV = 32
LEVELS = 4
TILE = 128
REPLICA_LIMIT = 16 * 2**20
VMEM_LIMIT = 40 * 2**20


def tile_products(source_rows, live_tiles, dest_slots, source_slots, row_tiles):
    source_tiles = source_rows.reshape(-1, 128, source_rows.shape[1])
    blocks = source_tiles[source_slots]
    products = jnp.einsum("src,sck->srk", live_tiles, blocks, preferred_element_type=jnp.float32)
    partial_value = jnp.zeros((row_tiles, 128, source_rows.shape[1]), jnp.float32)
    partial_value = partial_value.at[dest_slots].add(products)
    return partial_value.reshape(row_tiles * 128, source_rows.shape[1])


def local(tile_weights, tile_pos, tile_total, root_ids):
    col_devices = lax.axis_size("col")
    row_index = lax.axis_index("row")
    col_index = lax.axis_index("col")
    tile_data = tile_weights[0, 0]
    positions = tile_pos[0, 0]
    slot_limit = tile_total[0, 0]
    slot_total = tile_data.shape[0]
    in_use = (jnp.arange(slot_total, dtype=jnp.int32) < slot_limit).astype(jnp.bfloat16)
    live_tiles = tile_data * in_use[:, None, None]
    dest_slots = positions[0]
    source_slots = positions[1]
    row_block = col_devices * PV
    row_tiles = row_block // 128
    state_start = (row_index * col_devices + col_index) * PV
    state_rows = PV
    vertex_ids = state_start + jnp.arange(state_rows, dtype=jnp.int32)
    is_root = vertex_ids[:, None] == root_ids[None, :]
    kept_weight = is_root.astype(jnp.float32)
    path_now = is_root.astype(jnp.bfloat16)
    hop_level = jnp.where(is_root, 0, LEVELS + 1).astype(jnp.int32)
    found_counts = []
    found_totals = []
    for level_num in range(LEVELS):
        own_front = path_now
        source_rows = lax.all_gather(own_front, "row", axis=0, tiled=True)
        partial_value = tile_products(source_rows, live_tiles, dest_slots, source_slots, row_tiles)
        arrived = lax.psum_scatter(
            partial_value.astype(jnp.bfloat16), "col", scatter_dimension=0, tiled=True
        ).astype(jnp.float32)
        newly = (arrived > 0) & (hop_level == LEVELS + 1)
        path_weight = jnp.where(newly, arrived, jnp.float32(0.0))
        hop_level = jnp.where(newly, jnp.int32(level_num + 1), hop_level)
        kept_weight = kept_weight + path_weight
        path_now = path_weight.astype(jnp.bfloat16)
        found_count = jnp.sum(newly.astype(jnp.float32), axis=0)
        found_total = jnp.sum(path_weight, axis=0)
        found_counts.append(found_count)
        found_totals.append(found_total)
    counts = jnp.stack(found_counts)
    totals = jnp.stack(found_totals)
    counts, totals = lax.psum((counts, totals), ("row", "col"))
    factor = counts / jnp.maximum(totals, 1.0)
    factor_table = jnp.concatenate(
        [jnp.ones((1, ROOTS), jnp.float32), factor, jnp.zeros((1, ROOTS), jnp.float32)], axis=0
    )
    scale = jnp.zeros_like(kept_weight)
    for level_num in range(LEVELS + 2):
        scale = scale + jnp.where(
            hop_level == level_num, factor_table[level_num][None, :], jnp.float32(0.0)
        )
    return (hop_level, kept_weight * scale, counts)


def unpack(packed, hop_out, share_out, counts_out):
    hop_out[...] = packed[pl.ds(0, PV)].astype(jnp.int32)
    share_out[...] = packed[pl.ds(PV, PV)]
    counts_out[...] = packed[pl.ds(2 * PV, LEVELS)]


def kernel(
    n_row, n_col, tiles_hbm, pos_hbm, total_hbm, roots_hbm, packed,
    tiles_ref, pos_ref, total_ref, roots_ref, load_sem, adj, front, hop, path, send_z, recv_z, send_n, recv_n, send_d, recv_d, send_s, recv_s, recv_sd,
):
    loads = [
        pltpu.make_async_copy(source, target, load_sem.at[index])
        for index, (source, target) in enumerate(
            ((tiles_hbm, tiles_ref), (pos_hbm, pos_ref), (total_hbm, total_ref), (roots_hbm, roots_ref))
        )
    ]
    for load in loads:
        load.start()
    r = lax.axis_index("row")
    c = lax.axis_index("col")
    z, core = c // 2, c % 2
    y, x = r // 2, r % 2
    row_x, row_y, row_d = y * 2 + (1 - x), (1 - y) * 2 + x, (1 - y) * 2 + (1 - x)
    rows = (row_x, row_y)
    depth = n_col // 2
    slots = tiles_ref.shape[0]
    row_block, col_block = adj.shape[2], adj.shape[3]
    half = row_block // 2
    roots = roots_ref.shape[1]
    steps = sorted(range(1, depth), key=lambda step: min(step, depth - step))
    order = [z] + [(z + step) % depth for step in steps]

    barrier = pltpu.get_barrier_semaphore()
    others = [(r, zz * 2 + core) for zz in order[1:]]
    others += [(row_x, c), (row_y, c), (r, z * 2 + 1 - core)]
    for device in others:
        pl.semaphore_signal(barrier, inc=1, device_id=device, device_id_type=pl.DeviceIdType.MESH)

    for load in loads:
        load.wait()
    for tr in range(row_block // TILE):
        for tc in range(col_block // TILE):
            value = jnp.zeros((TILE, TILE), jnp.float32)
            for s in range(slots):
                here = (pos_ref[0, s] == tr) & (pos_ref[1, s] == tc) & (s < total_ref[0, 0])
                value = value + tiles_ref[s].astype(jnp.float32) * here.astype(jnp.float32)
            adj[c, r, pl.ds(tr * TILE, TILE), pl.ds(tc * TILE, TILE)] = value.astype(jnp.bfloat16)

    pl.semaphore_wait(barrier, len(others))

    started = []

    def send(ref, send_sem, recv_sem, device):
        copy = pltpu.make_async_remote_copy(
            src_ref=ref, dst_ref=ref, send_sem=send_sem, recv_sem=recv_sem,
            device_id=device, device_id_type=pl.DeviceIdType.MESH,
        )
        copy.start()
        started.append(copy)

    def arrive(ref, send_sem, recv_sem):
        pltpu.make_async_remote_copy(
            src_ref=ref, dst_ref=ref, send_sem=send_sem, recv_sem=recv_sem,
            device_id=(r, z * 2 + 1 - core), device_id_type=pl.DeviceIdType.MESH,
        ).wait_recv()

    def block(zz, rr):
        return adj.at[zz * 2 + core, rr]

    def piece(zz, rr, h):
        return adj.at[zz * 2 + core, rr, pl.ds(h * half, half)]

    sibling = (r, z * 2 + 1 - core)

    def spread(zz):
        for turn in range(2):
            for axis in range(2):
                h = axis if turn == 0 else 1 - axis
                send(piece(zz, r, h), send_n.at[axis, h, zz], recv_n.at[axis, h, zz], (rows[axis], c))

    def share_block(zz, rr):
        send(block(zz, rr), send_s.at[rr, zz], recv_s.at[rr, zz], sibling)

    def relay(zz):
        for axis in range(2):
            arrive(piece(zz, rows[axis], axis), send_n.at[axis, axis, zz], recv_n.at[axis, axis, zz])
            send(piece(zz, rows[axis], axis), send_d.at[axis, zz], recv_d.at[axis, zz], (rows[1 - axis], c))
        for axis in range(2):
            arrive(piece(zz, rows[axis], 1 - axis), send_n.at[axis, 1 - axis, zz], recv_n.at[axis, 1 - axis, zz])
            share_block(zz, rows[axis])

    def finish(zz):
        for axis in range(2):
            arrive(piece(zz, row_d, axis), send_d.at[axis, zz], recv_d.at[axis, zz])
            send(piece(zz, row_d, axis), send_s.at[n_row + axis, zz], recv_sd.at[axis, zz], sibling)

    spread(z)
    for step in range(depth - 1):
        zz = order[step + 1]
        send(block(z, r), send_z.at[zz], recv_z.at[z], (r, zz * 2 + core))
    share_block(z, r)
    for rr in range(n_row):
        part = pl.ds(rr * row_block, row_block)
        ids = rr * row_block + lax.broadcasted_iota(jnp.int32, (row_block, roots), 0)
        is_root = ids == roots_ref[...]
        hop[part] = jnp.where(is_root, 0, LEVELS + 1).astype(jnp.int32)
        path[part] = is_root.astype(jnp.float32)
        for cc in range(n_col):
            front[0, pl.ds(cc * col_block + rr * PV, PV)] = (
                is_root[cc * PV:(cc + 1) * PV].astype(jnp.float32).astype(jnp.bfloat16)
            )
    for step in range(depth):
        if step + 1 < depth:
            zz = order[step + 1]
            arrive(block(zz, r), send_z.at[zz], recv_z.at[zz])
            spread(zz)
            share_block(zz, r)
        relay(order[step])
        if step > 0:
            finish(order[step - 1])
    finish(order[depth - 1])
    for step in range(depth):
        zz = order[step]
        for rr in (r, row_x, row_y):
            arrive(adj.at[zz * 2 + 1 - core, rr], send_s.at[rr, zz], recv_s.at[rr, zz])
        for axis in range(2):
            arrive(
                adj.at[zz * 2 + 1 - core, row_d, pl.ds(axis * half, half)],
                send_s.at[n_row + axis, zz], recv_sd.at[axis, zz],
            )

    own = pl.ds(pl.multiple_of((r * n_col + c) * PV, PV), PV)
    kept = path[own]
    factors = []
    for level in range(LEVELS):
        now, later = level % 2, (level + 1) % 2
        count = jnp.zeros((1, roots), jnp.float32)
        total = jnp.zeros((1, roots), jnp.float32)
        source = front[now]
        for rr in range(n_row):
            part = pl.ds(rr * row_block, row_block)
            wide = jnp.concatenate([adj[cc, rr] for cc in range(n_col)], axis=1)
            arrived = jnp.dot(wide, source, preferred_element_type=jnp.float32)
            old = hop[part]
            newly = (arrived > 0) & (old == LEVELS + 1)
            weight = jnp.where(newly, arrived, 0.0)
            hop[part] = jnp.where(newly, level + 1, old)
            path[part] = weight
            count = count + jnp.sum(newly.astype(jnp.float32), axis=0, keepdims=True)
            total = total + jnp.sum(weight, axis=0, keepdims=True)
            narrow = weight.astype(jnp.bfloat16)
            if level + 1 < LEVELS:
                for cc in range(n_col):
                    front[later, pl.ds(cc * col_block + rr * PV, PV)] = narrow[cc * PV:(cc + 1) * PV]
        kept = kept + path[own]
        packed[pl.ds(2 * PV + level, 1)] = count
        factors.append(count / jnp.maximum(total, 1.0))
    level_own = hop[own]
    scale = jnp.where(level_own == 0, 1.0, 0.0)
    for level in range(LEVELS):
        scale = jnp.where(level_own == level + 1, factors[level], scale)
    packed[pl.ds(0, PV)] = level_own.astype(jnp.float32)
    packed[pl.ds(PV, PV)] = kept * scale

    for copy in started:
        copy.wait_send()


def replicated(n_row, n_col, tile_weights, tile_pos, tile_total, root_ids):
    roots = root_ids.shape[0]
    row_block, col_block = n_col * PV, n_row * PV
    vertices = n_row * row_block
    depth = n_col // 2
    vmem = pl.BlockSpec(memory_space=pltpu.VMEM)
    hbm = pl.BlockSpec(memory_space=pltpu.HBM)
    dma = pltpu.SemaphoreType.DMA
    packed = pl.pallas_call(
        functools.partial(kernel, n_row, n_col),
        out_shape=jax.ShapeDtypeStruct((2 * PV + LEVELS, roots), jnp.float32),
        in_specs=[hbm, hbm, hbm, hbm],
        out_specs=vmem,
        scratch_shapes=[
            pltpu.VMEM(tile_weights.shape[2:], tile_weights.dtype),
            pltpu.SMEM(tile_pos.shape[2:], jnp.int32),
            pltpu.SMEM(tile_total.shape, jnp.int32),
            pltpu.VMEM((1, roots), jnp.int32),
            dma((4,)),
            pltpu.VMEM((n_col, n_row, row_block, col_block), jnp.bfloat16),
            pltpu.VMEM((2, vertices, roots), jnp.bfloat16),
            pltpu.VMEM((vertices, roots), jnp.int32),
            pltpu.VMEM((vertices, roots), jnp.float32),
            dma((depth,)), dma((depth,)),
            dma((2, 2, depth)), dma((2, 2, depth)),
            dma((2, depth)), dma((2, depth)),
            dma((n_row + 2, depth)), dma((n_row, depth)), dma((2, depth)),
        ],
        compiler_params=pltpu.CompilerParams(collective_id=0, has_side_effects=True, vmem_limit_bytes=VMEM_LIMIT),
    )(tile_weights[0, 0], tile_pos[0, 0], tile_total, root_ids.reshape(1, roots))
    return pl.pallas_call(
        unpack,
        out_shape=(
            jax.ShapeDtypeStruct((PV, roots), jnp.int32),
            jax.ShapeDtypeStruct((PV, roots), jnp.float32),
            jax.ShapeDtypeStruct((LEVELS, roots), jnp.float32),
        ),
        in_specs=[vmem],
        out_specs=(vmem, vmem, vmem),
        compiler_params=pltpu.CompilerParams(vmem_limit_bytes=2**20),
    )(packed)


def solution(mesh):
    n_row, n_col = mesh.shape["row"], mesh.shape["col"]
    vertices = n_row * n_col * PV
    placed = (P("row", "col", None, None, None), P("row", "col", None, None), P("row", "col"), P())
    body = local
    if n_row == 4 and n_col % 2 == 0 and 2 * vertices * vertices <= REPLICA_LIMIT:
        body = functools.partial(replicated, n_row, n_col)
    return jax.shard_map(
        body,
        mesh=mesh,
        in_specs=placed,
        out_specs=(P(("row", "col"), None), P(("row", "col"), None), P()),
        check_vma=False,
    )
```
